32 devices in a mesh: span: 4 (over y, x), model: 8 (over z, core).
Axes of the slice: x: 2, y: 2, z: 4, core: 2. Of those that a mesh axis runs over, the one named last changes fastest.
Arguments:
- latents: bfloat16 [4, 2048, 512], P(None, ('span', 'model')), may hold values from -6 to 6
- rotary_rows: bfloat16 [4, 2048, 64], P(None, ('span', 'model')), may hold values from -6 to 6
- latent_gain: float32 [512], replicated, may hold values from 0.25 to 1.75
- key_up: bfloat16 [512, 16, 128], P(None, 'model'), may hold values from -0.25 to 0.25
- value_up: bfloat16 [512, 16, 128], P(None, 'model'), may hold values from -0.25 to 0.25
Outputs:
- decode_keys: bfloat16 [4, 16, 192, 2048], P('span', 'model')
- decode_values: bfloat16 [4, 2048, 16, 128], P('span', None, 'model')
The draws below stay inside these ranges and needn't reach their ends.
All inputs are finite; a program needn't handle non-finite values.
Results may differ from the reference program's by a relative error of at most 0.0049.
Values may be sent and summed in bfloat16 or wider, within the bound.
No kernel may reach another device: no remote copies, remote signals or barrier semaphores. Data moves between devices by JAX's collectives and lax.ppermute only.
A program may use at most 64 MiB of HBM per device.

```python
import jax
import jax.numpy as jnp
from jax import lax

BATCH = 4
LENGTH = 2048
HEADS = 16
LATENT = 512
KEY_PART = 128
ROTARY = 64
VALUE_SIZE = 128


def block_levels(own_key, dims, pieces, smallest, high):
    factor_of, own = 1.0, jax.random.fold_in(own_key, 6)
    for dim, shards_of in pieces:
        heights = jnp.exp(jax.random.uniform(jax.random.fold_in(own, dim), (shards_of,), jnp.float32, smallest / len(pieces), high / len(pieces)))
        factor_of = factor_of * jnp.repeat(heights, dims[dim] // shards_of).reshape([-1 if axis == dim else 1 for axis in range(len(dims))])
    return factor_of


def normal_values(own_key, shape, scale, most, cuts=(), dtype=jnp.bfloat16):
    loudness = block_levels(own_key, shape, cuts, -0.22, 0.18) if cuts else 1.0
    entries = jax.random.normal(own_key, shape, jnp.float32) * scale * loudness
    return jnp.minimum(jnp.maximum(entries, -most), most).astype(dtype)


def setup_inputs(seed: int = 0) -> dict:
    streams_of = jax.random.split(jax.random.key(seed), 6)
    return {
        "latents": normal_values(streams_of[0], (BATCH, LENGTH, LATENT), 1.0, 6.0, ((1, 32),)),
        "rotary_rows": normal_values(streams_of[1], (BATCH, LENGTH, ROTARY), 1.0, 6.0, ((1, 32),)),
        "latent_gain": jnp.clip(1.0 + 0.15 * jax.random.normal(streams_of[2], (LATENT,), jnp.float32), 0.25, 1.75),
        "key_up": normal_values(streams_of[3], (LATENT, HEADS, KEY_PART), LATENT ** -0.5, 0.25, ((1, 8),)),
        "value_up": normal_values(streams_of[4], (LATENT, HEADS, VALUE_SIZE), LATENT ** -0.5, 0.25, ((1, 8),)),
    }


def scale_rows(vectors, row_gain):
    return vectors * lax.rsqrt(lax.optimization_barrier(jnp.mean(vectors * vectors, axis=-1, keepdims=True)) + 1e-06) * row_gain

def reference(latents, rotary_rows, latent_gain, key_up, value_up):
    rows_ready = scale_rows(latents.astype(jnp.float32), latent_gain).astype(jnp.bfloat16)
    rows_ready = lax.optimization_barrier(rows_ready)

    def expand_one(one):
        rows_one, rotary_one = one
        wide_keys = jnp.einsum('tr,rhk->thk', rows_one.astype(jnp.float32), key_up.astype(jnp.float32)).astype(jnp.bfloat16)
        shared = jnp.broadcast_to(rotary_one[:, None], (LENGTH, HEADS, ROTARY))
        wide_values = jnp.einsum('tr,rhk->thk', rows_one.astype(jnp.float32), value_up.astype(jnp.float32)).astype(jnp.bfloat16)
        return (jnp.concatenate([wide_keys, shared], axis=-1), wide_values)
    decode_keys, decode_values = lax.map(expand_one, (rows_ready, rotary_rows))
    decode_keys = jnp.transpose(decode_keys, (0, 2, 3, 1))
    return (decode_keys, decode_values)
```

```python
import jax
import jax.numpy as jnp
from jax import lax
from jax.experimental import pallas as pl
from jax.experimental.pallas import tpu as pltpu
from jax.sharding import PartitionSpec as P

LANES = 128
CHUNKS = 2


def pack_rows(latents, rotary, latent_gain):
    seqs, count, width = latents.shape
    rot = rotary.shape[2]
    fold = LANES // rot
    pieces = width // LANES
    high = pieces * count + count // fold

    def body(rows_ref, rotary_ref, gain_ref, out_ref):
        for s in range(seqs):
            rows = rows_ref[s].astype(jnp.float32)
            scale = lax.rsqrt(jnp.mean(rows * rows, axis=-1, keepdims=True) + 1e-06)
            ready = (rows * scale * gain_ref[...]).astype(jnp.bfloat16)
            for i in range(pieces):
                out_ref[s, i * count : (i + 1) * count] = ready[:, i * LANES : (i + 1) * LANES]
            part = rotary_ref[s].astype(jnp.float32)
            cut = count // fold
            wide = jnp.concatenate([part[i * cut : (i + 1) * cut] for i in range(fold)], axis=1)
            out_ref[s, pieces * count :] = wide.astype(jnp.bfloat16)

    return pl.pallas_call(
        body,
        out_shape=jax.ShapeDtypeStruct((seqs, high, LANES), jnp.bfloat16),
        name="pack",
    )(latents, rotary, latent_gain.reshape(1, -1))


def expand(order, chunks, keys_t, values, count, rot, width, spans, core):
    heads = values.shape[1]
    key_part = keys_t.shape[0] // heads
    value_size = values.shape[2]
    values = values.reshape(width, heads * value_size)
    zs, _, high, _ = chunks[0][0].shape
    cores = len(chunks[0])
    tile = zs * cores * count
    pieces, fold = width // LANES, LANES // rot
    cut = count // fold
    starts = [0]
    for chunk in chunks:
        starts.append(starts[-1] + chunk[0].shape[1])
    refs_of = len(chunks) * cores

    def body(order_ref, *refs):
        ins, (key_ref, value_ref, keys_out, values_out, rows_s, rot_s, wide_s) = (
            refs[:refs_of],
            refs[refs_of:],
        )
        step = pl.program_id(0)
        first = order_ref[spans] == 0

        for j in range(len(chunks)):

            @pl.when((step >= starts[j]) & (step < starts[j + 1]))
            def _(j=j):
                pair = ins[j * cores : (j + 1) * cores]
                for z in range(zs):
                    got = [ref[z, 0] for ref in pair]
                    if cores == 2:
                        got = [
                            jnp.where(first, got[0], got[1]),
                            jnp.where(first, got[1], got[0]),
                        ]
                    for c in range(cores):
                        at = (z * cores + c) * count
                        for i in range(pieces):
                            rows_s[at : at + count, i * LANES : (i + 1) * LANES] = got[c][
                                i * count : (i + 1) * count
                            ]
                        tail = got[c][pieces * count :].astype(jnp.float32)
                        for i in range(fold):
                            rot_s[at + i * cut : at + (i + 1) * cut] = tail[
                                :, i * rot : (i + 1) * rot
                            ].astype(jnp.bfloat16)

        rows = rows_s[...]
        dims = (((1,), (1,)), ((), ()))
        wide_keys = lax.dot_general(key_ref[...], rows, dims, preferred_element_type=jnp.float32)
        wide_keys = wide_keys.astype(jnp.bfloat16)
        eye = (
            lax.broadcasted_iota(jnp.int32, (rot, rot), 0)
            == lax.broadcasted_iota(jnp.int32, (rot, rot), 1)
        ).astype(jnp.float32).astype(jnp.bfloat16)
        shared = lax.dot_general(eye, rot_s[...], dims, preferred_element_type=jnp.float32)
        shared = shared.astype(jnp.bfloat16)
        for h in range(heads):
            keys_out[0, h, :key_part] = wide_keys[h * key_part : (h + 1) * key_part]
            keys_out[0, h, key_part:] = shared
        wide_values = jnp.dot(rows, value_ref[...], preferred_element_type=jnp.float32)
        if heads == 1:
            values_out[...] = wide_values.astype(jnp.bfloat16)
        else:
            for h in range(heads):
                wide_s[pl.ds(h, tile, stride=heads)] = wide_values[
                    :, h * value_size : (h + 1) * value_size
                ]
            values_out[...] = wide_s[...].astype(jnp.bfloat16)

    length = spans * tile
    specs = []
    for j, chunk in enumerate(chunks):
        most = chunk[0].shape[1] - 1
        for _ in chunk:
            specs.append(
                pl.BlockSpec(
                    (zs, 1, high, LANES),
                    lambda i, o, a=starts[j], m=most: (0, jnp.clip(i - a, 0, m), 0, 0),
                )
            )
    whole = lambda i, o: (0, 0)
    decode_keys, decode_values = pl.pallas_call(
        body,
        grid_spec=pltpu.PrefetchScalarGridSpec(
            num_scalar_prefetch=1,
            grid=(spans,),
            in_specs=specs
            + [pl.BlockSpec(keys_t.shape, whole), pl.BlockSpec(values.shape, whole)],
            out_specs=[
                pl.BlockSpec((1, heads, key_part + rot, tile), lambda i, o: (0, 0, 0, o[i])),
                pl.BlockSpec((tile * heads, value_size), lambda i, o: (o[i], 0)),
            ],
            scratch_shapes=[
                pltpu.VMEM((tile, width), jnp.bfloat16),
                pltpu.VMEM((tile, rot), jnp.bfloat16),
                pltpu.VMEM((tile * heads, value_size), jnp.float32),
            ],
        ),
        out_shape=[
            jax.ShapeDtypeStruct((1, heads, key_part + rot, length), jnp.bfloat16),
            jax.ShapeDtypeStruct((length * heads, value_size), jnp.bfloat16),
        ],
        name="expand",
    )(order, *[a for chunk in chunks for a in chunk], keys_t, values)
    return decode_keys, decode_values.reshape(1, length, heads, value_size)


def shards(latents, rotary_rows, latent_gain, key_up, value_up):
    spans, models = lax.axis_size("span"), lax.axis_size("model")
    me, place = lax.axis_index("span"), lax.axis_index("model")
    _, count, width = latents.shape
    rot = rotary_rows.shape[2]
    cores = 2
    core = place % cores
    packed = pack_rows(latents, rotary_rows, latent_gain)
    keys_t = key_up.transpose(1, 2, 0).reshape(-1, width)

    parts = [lax.dynamic_slice_in_dim(packed, me, 1, 0)]
    for k in range(1, spans):
        sent = lax.dynamic_slice_in_dim(packed, me ^ k, 1, 0)
        parts.append(lax.ppermute(sent, "span", [(i, i ^ k) for i in range(spans)]))
    order = jnp.concatenate(
        [me ^ jnp.arange(spans, dtype=jnp.int32), core.astype(jnp.int32)[None]]
    )

    along = [[z * cores + c for z in range(models // cores)] for c in range(cores)]
    swap = [(i, i ^ 1) for i in range(models)]
    chunks, size = [], spans // CHUNKS
    token = None
    for j in range(CHUNKS):
        mine = jnp.concatenate(parts[j * size : (j + 1) * size], axis=0)
        if token is not None:
            mine, _ = lax.optimization_barrier((mine, token))
        own = lax.all_gather(mine, "model", axis_index_groups=along)
        token = own
        chunks.append((own, lax.ppermute(own, "model", swap)))
    return expand(order, chunks, keys_t, value_up, count, rot, width, spans, core)


def solution(mesh):
    placed = (
        P(None, ("span", "model"), None),
        P(None, ("span", "model"), None),
        P(),
        P(None, "model", None),
        P(None, "model", None),
    )
    return jax.shard_map(
        shards,
        mesh=mesh,
        in_specs=placed,
        out_specs=(P("span", "model", None, None), P("span", None, "model", None)),
        check_vma=False,
    )
```

```python
import jax
import jax.numpy as jnp
from jax import lax
from jax.experimental import pallas as pl
from jax.experimental.pallas import tpu as pltpu
from jax.sharding import PartitionSpec as P


LANES = 128
CORES = 2
CHUNKS = 1
VMEM = pl.BlockSpec(memory_space=pltpu.VMEM)
HBM = pl.BlockSpec(memory_space=pl.ANY)


def pack_rows(latents, rotary, latent_gain, spans):
    _, count, width = latents.shape
    rot = rotary.shape[2]
    fold = LANES // rot
    pieces = width // LANES
    high = pieces * count + count // fold
    cut = count // fold

    def body(rows_ref, rotary_ref, gain_ref, *outs):
        me = lax.axis_index("span")
        for k in range(spans):
            rows = rows_ref[me ^ k].astype(jnp.float32)
            scale = lax.rsqrt(jnp.mean(rows * rows, axis=-1, keepdims=True) + 1e-06)
            ready = (rows * scale * gain_ref[...]).astype(jnp.bfloat16)
            for i in range(pieces):
                outs[k][0, i * count : (i + 1) * count] = ready[:, i * LANES : (i + 1) * LANES]
            part = rotary_ref[me ^ k].astype(jnp.float32)
            wide = jnp.concatenate([part[i * cut : (i + 1) * cut] for i in range(fold)], axis=1)
            outs[k][0, pieces * count :] = wide.astype(jnp.bfloat16)

    return pl.pallas_call(
        body,
        in_specs=[VMEM] * 3,
        out_specs=[VMEM] * spans,
        out_shape=[jax.ShapeDtypeStruct((1, high, LANES), jnp.bfloat16)] * spans,
        name="pack",
    )(latents, rotary, latent_gain.reshape(1, -1))


def expand(slots, before, keys_t, values, shape, last):
    heads, key_part, value_size, count, rot, width, spans, zs = shape
    pieces, fold = width // LANES, LANES // rot
    cut = count // fold
    tile = CORES * count
    every = spans * tile
    arrays = [a for _, chunks in slots for pair in chunks for a in pair]
    count_in = len(arrays) + 2 + len(before)

    def body(*refs):
        ins, keys_ref, value_ref = refs[: len(arrays)], refs[len(arrays)], refs[len(arrays) + 1]
        keys_out, values_out, rows_s, rot_s, wide_s, key_s, value_s, sems = refs[count_in:]
        me, place = lax.axis_index("span"), lax.axis_index("model")
        z, first = place // CORES, (place % CORES) == 0

        def block(s, k):
            return (me ^ k) * zs + z + slots[s][0]

        def key_copies(s):
            for k in range(spans):
                at = pl.multiple_of(block(s, k) * tile, tile)
                to = keys_out.at[0, :, :, pl.ds(at, tile)]
                yield pltpu.make_async_copy(key_s.at[s, k], to, sems.at[s, k, 0])

        def value_copies(s):
            for k in range(spans):
                at = pl.multiple_of(block(s, k) * tile * heads, tile * heads)
                to = values_out.at[pl.ds(at, tile * heads)]
                yield pltpu.make_async_copy(value_s.at[s, k], to, sems.at[s, k, 1])

        def work(s, base):
            k = 0
            for j, chunk in enumerate(slots[s][1]):
                own, other = ins[base + 2 * j], ins[base + 2 * j + 1]
                for b in range(chunk[0].shape[0]):
                    mine, theirs = own[b], other[b]
                    got = (jnp.where(first, mine, theirs), jnp.where(first, theirs, mine))
                    for c in range(CORES):
                        at = (k * CORES + c) * count
                        for i in range(pieces):
                            rows_s[at : at + count, i * LANES : (i + 1) * LANES] = got[c][
                                i * count : (i + 1) * count
                            ]
                        tail = got[c][pieces * count :].astype(jnp.float32)
                        for i in range(fold):
                            rot_s[at + i * cut : at + (i + 1) * cut] = tail[
                                :, i * rot : (i + 1) * rot
                            ].astype(jnp.bfloat16)
                    k += 1
            rows = rows_s[...]
            dims = (((1,), (1,)), ((), ()))
            wide_keys = lax.dot_general(keys_ref[...], rows, dims, preferred_element_type=jnp.float32)
            wide_keys = wide_keys.astype(jnp.bfloat16)
            eye = (
                lax.broadcasted_iota(jnp.int32, (rot, rot), 0)
                == lax.broadcasted_iota(jnp.int32, (rot, rot), 1)
            ).astype(jnp.float32).astype(jnp.bfloat16)
            shared = lax.dot_general(eye, rot_s[...], dims, preferred_element_type=jnp.float32)
            shared = shared.astype(jnp.bfloat16)
            for k in range(spans):
                lanes = slice(k * tile, (k + 1) * tile)
                for h in range(heads):
                    key_s[s, k, h, :key_part] = wide_keys[h * key_part : (h + 1) * key_part, lanes]
                    key_s[s, k, h, key_part:] = shared[:, lanes]
            for copy in key_copies(s):
                copy.start()
            wide_values = jnp.dot(rows, value_ref[...], preferred_element_type=jnp.float32)
            for h in range(heads):
                wide_s[pl.ds(h, every, stride=heads)] = wide_values[
                    :, h * value_size : (h + 1) * value_size
                ]
            for k in range(spans):
                value_s[s, k] = wide_s[k * tile * heads : (k + 1) * tile * heads].astype(jnp.bfloat16)
            for copy in value_copies(s):
                copy.start()

        base = 0
        for s, (offset, chunks) in enumerate(slots):
            there = (z + offset >= 0) & (z + offset < zs)
            pl.when(there)(lambda s=s, base=base: work(s, base))
            base += 2 * len(chunks)
        for s, (offset, _) in enumerate(slots):
            there = (z + offset >= 0) & (z + offset < zs)

            @pl.when(there)
            def _(s=s):
                for copy in (*key_copies(s), *value_copies(s)):
                    copy.wait()

    length = every * zs
    given = (*arrays, keys_t, values)
    if last:
        given = [pltpu.with_memory_space_constraint(a, pltpu.VMEM) for a in given]
    return pl.pallas_call(
        body,
        in_specs=[VMEM] * (len(arrays) + 2) + [HBM] * len(before),
        out_specs=[HBM, HBM],
        out_shape=[
            jax.ShapeDtypeStruct((1, heads, key_part + rot, length), jnp.bfloat16),
            jax.ShapeDtypeStruct((length * heads, value_size), jnp.bfloat16),
        ],
        scratch_shapes=[
            pltpu.VMEM((every, width), jnp.bfloat16),
            pltpu.VMEM((every, rot), jnp.bfloat16),
            pltpu.VMEM((every * heads, value_size), jnp.float32),
            pltpu.VMEM((len(slots), spans, heads, key_part + rot, tile), jnp.bfloat16),
            pltpu.VMEM((len(slots), spans, tile * heads, value_size), jnp.bfloat16),
            pltpu.SemaphoreType.DMA((len(slots), spans, 2)),
        ],
        input_output_aliases={len(arrays) + 2 + i: i for i in range(len(before))},
    )(*given, *before)


def expand_spans(order, chunks, keys_t, values, count, rot, width, spans):
    heads = values.shape[1]
    key_part = keys_t.shape[0] // heads
    value_size = values.shape[2]
    values = values.reshape(width, heads * value_size)
    zs, _, high, _ = chunks[0][0].shape
    cores = len(chunks[0])
    tile = zs * cores * count
    pieces, fold = width // LANES, LANES // rot
    cut = count // fold
    starts = [0]
    for chunk in chunks:
        starts.append(starts[-1] + chunk[0].shape[1])
    refs_of = len(chunks) * cores

    def body(order_ref, *refs):
        ins, (key_ref, value_ref, keys_out, values_out, rows_s, rot_s, wide_s) = (
            refs[:refs_of],
            refs[refs_of:],
        )
        step = pl.program_id(0)
        first = order_ref[spans] == 0

        for j in range(len(chunks)):

            @pl.when((step >= starts[j]) & (step < starts[j + 1]))
            def _(j=j):
                pair = ins[j * cores : (j + 1) * cores]
                for z in range(zs):
                    got = [ref[z, 0] for ref in pair]
                    if cores == 2:
                        got = [
                            jnp.where(first, got[0], got[1]),
                            jnp.where(first, got[1], got[0]),
                        ]
                    for c in range(cores):
                        at = (z * cores + c) * count
                        for i in range(pieces):
                            rows_s[at : at + count, i * LANES : (i + 1) * LANES] = got[c][
                                i * count : (i + 1) * count
                            ]
                        tail = got[c][pieces * count :].astype(jnp.float32)
                        for i in range(fold):
                            rot_s[at + i * cut : at + (i + 1) * cut] = tail[
                                :, i * rot : (i + 1) * rot
                            ].astype(jnp.bfloat16)

        rows = rows_s[...]
        dims = (((1,), (1,)), ((), ()))
        wide_keys = lax.dot_general(key_ref[...], rows, dims, preferred_element_type=jnp.float32)
        wide_keys = wide_keys.astype(jnp.bfloat16)
        eye = (
            lax.broadcasted_iota(jnp.int32, (rot, rot), 0)
            == lax.broadcasted_iota(jnp.int32, (rot, rot), 1)
        ).astype(jnp.float32).astype(jnp.bfloat16)
        shared = lax.dot_general(eye, rot_s[...], dims, preferred_element_type=jnp.float32)
        shared = shared.astype(jnp.bfloat16)
        for h in range(heads):
            keys_out[0, h, :key_part] = wide_keys[h * key_part : (h + 1) * key_part]
            keys_out[0, h, key_part:] = shared
        wide_values = jnp.dot(rows, value_ref[...], preferred_element_type=jnp.float32)
        if heads == 1:
            values_out[...] = wide_values.astype(jnp.bfloat16)
        else:
            for h in range(heads):
                wide_s[pl.ds(h, tile, stride=heads)] = wide_values[
                    :, h * value_size : (h + 1) * value_size
                ]
            values_out[...] = wide_s[...].astype(jnp.bfloat16)

    length = spans * tile
    specs = []
    for j, chunk in enumerate(chunks):
        most = chunk[0].shape[1] - 1
        for _ in chunk:
            specs.append(
                pl.BlockSpec(
                    (zs, 1, high, LANES),
                    lambda i, o, a=starts[j], m=most: (0, jnp.clip(i - a, 0, m), 0, 0),
                )
            )
    whole = lambda i, o: (0, 0)
    decode_keys, decode_values = pl.pallas_call(
        body,
        grid_spec=pltpu.PrefetchScalarGridSpec(
            num_scalar_prefetch=1,
            grid=(spans,),
            in_specs=specs
            + [pl.BlockSpec(keys_t.shape, whole), pl.BlockSpec(values.shape, whole)],
            out_specs=[
                pl.BlockSpec((1, heads, key_part + rot, tile), lambda i, o: (0, 0, 0, o[i])),
                pl.BlockSpec((tile * heads, value_size), lambda i, o: (o[i], 0)),
            ],
            scratch_shapes=[
                pltpu.VMEM((tile, width), jnp.bfloat16),
                pltpu.VMEM((tile, rot), jnp.bfloat16),
                pltpu.VMEM((tile * heads, value_size), jnp.float32),
            ],
        ),
        out_shape=[
            jax.ShapeDtypeStruct((1, heads, key_part + rot, length), jnp.bfloat16),
            jax.ShapeDtypeStruct((length * heads, value_size), jnp.bfloat16),
        ],
        name="expand_spans",
    )(order, *[a for chunk in chunks for a in chunk], keys_t, values)
    return decode_keys, decode_values.reshape(1, length, heads, value_size)


def decode(latents, rotary_rows, latent_gain, key_up, value_up):
    spans, models = lax.axis_size("span"), lax.axis_size("model")
    zs = models // CORES
    _, count, width = latents.shape
    rot = rotary_rows.shape[2]
    heads, key_part, value_size = key_up.shape[1], key_up.shape[2], value_up.shape[2]
    shape = (heads, key_part, value_size, count, rot, width, spans, zs)
    packed = pack_rows(latents, rotary_rows, latent_gain, spans)
    keys_t = key_up.transpose(1, 2, 0).reshape(-1, width)
    values = value_up.reshape(width, heads * value_size)
    swap = [(i, i ^ 1) for i in range(models)]

    parts = [packed[0]]
    for k in range(1, spans):
        parts.append(lax.ppermute(packed[k], "span", [(i, i ^ k) for i in range(spans)]))
    size = spans // CHUNKS
    keys_t, values, *parts[1:] = lax.optimization_barrier((keys_t, values, *parts[1:]))
    if (CORES * count) % LANES:
        me, place = lax.axis_index("span"), lax.axis_index("model")
        core = place % CORES
        order = jnp.concatenate(
            [me ^ jnp.arange(spans, dtype=jnp.int32), core.astype(jnp.int32)[None]]
        )
        along = [[z * CORES + c for z in range(zs)] for c in range(CORES)]
        mine = jnp.concatenate(parts, axis=0)
        own = lax.all_gather(mine, "model", axis_index_groups=along)
        chunks = [(own, lax.ppermute(own, "model", swap))]
        return expand_spans(order, chunks, keys_t, value_up, count, rot, width, spans)
    own = [jnp.concatenate(parts[j * size : (j + 1) * size], axis=0) for j in range(CHUNKS)]

    def hop(x, way, far):
        pairs = []
        for z in range(zs):
            if 0 <= z + way < zs and 0 <= z - way * far < zs:
                for c in range(CORES):
                    pairs.append((z * CORES + c, (z + way) * CORES + c))
        return lax.ppermute(x, "model", pairs)

    def paired(x):
        return (x, lax.ppermute(x, "model", swap))

    slots = [[(0, [paired(x) for x in own])]]
    moving = {1: own, -1: own}
    for d in range(1, zs):
        for way in (1, -1):
            moving[way] = [hop(x, way, d - 1) for x in moving[way]]
        slots.append([(-way * d, [paired(x) for x in moving[way]]) for way in (1, -1)])
    groups = [sum(slots[:-1], []), slots[-1]]
    outs = ()
    for n, group in enumerate(groups):
        outs = expand(group, outs, keys_t, values, shape, n == 1)
    decode_keys, decode_values = outs
    return decode_keys, decode_values.reshape(1, -1, heads, value_size)


def solution(mesh):
    placed = (
        P(None, ("span", "model"), None),
        P(None, ("span", "model"), None),
        P(),
        P(None, "model", None),
        P(None, "model", None),
    )
    return jax.shard_map(
        decode,
        mesh=mesh,
        in_specs=placed,
        out_specs=(P("span", "model", None, None), P("span", None, "model", None)),
        check_vma=False,
    )
```

```python
import jax
import jax.numpy as jnp
from jax import lax
from jax.experimental import pallas as pl
from jax.experimental.pallas import tpu as pltpu
from jax.sharding import PartitionSpec as P


LANES = 128
CORES = 2
CHUNKS = 1
VMEM = pl.BlockSpec(memory_space=pltpu.VMEM)
HBM = pl.BlockSpec(memory_space=pl.ANY)


def pack_rows(latents, rotary, latent_gain, spans):
    _, count, width = latents.shape
    rot = rotary.shape[2]
    fold = LANES // rot
    pieces = width // LANES
    high = pieces * count + count // fold
    cut = count // fold

    def body(rows_ref, rotary_ref, gain_ref, *outs):
        me = lax.axis_index("span")
        for k in range(spans):
            rows = rows_ref[me ^ k].astype(jnp.float32)
            scale = lax.rsqrt(jnp.mean(rows * rows, axis=-1, keepdims=True) + 1e-06)
            ready = (rows * scale * gain_ref[...]).astype(jnp.bfloat16)
            for i in range(pieces):
                outs[k][0, i * count : (i + 1) * count] = ready[:, i * LANES : (i + 1) * LANES]
            part = rotary_ref[me ^ k].astype(jnp.float32)
            wide = jnp.concatenate([part[i * cut : (i + 1) * cut] for i in range(fold)], axis=1)
            outs[k][0, pieces * count :] = wide.astype(jnp.bfloat16)

    return pl.pallas_call(
        body,
        in_specs=[VMEM] * 3,
        out_specs=[VMEM] * spans,
        out_shape=[jax.ShapeDtypeStruct((1, high, LANES), jnp.bfloat16)] * spans,
        name="pack",
    )(latents, rotary, latent_gain.reshape(1, -1))


def expand(slots, before, keys_t, values, shape, last):
    heads, key_part, value_size, count, rot, width, spans, zs = shape
    pieces, fold = width // LANES, LANES // rot
    cut = count // fold
    tile = CORES * count
    every = spans * tile
    arrays = [a for _, chunks in slots for pair in chunks for a in pair]
    count_in = len(arrays) + 2 + len(before)

    def body(*refs):
        ins, keys_ref, value_ref = refs[: len(arrays)], refs[len(arrays)], refs[len(arrays) + 1]
        keys_out, values_out, rows_s, rot_s, wide_s, key_s, value_s, sems = refs[count_in:]
        me, place = lax.axis_index("span"), lax.axis_index("model")
        z, first = place // CORES, (place % CORES) == 0

        def offset_of(s):
            offset = slots[s][0]
            if isinstance(offset, int):
                return offset
            return jnp.where(z + offset[0] >= 0, offset[0], offset[1])

        def block(s, k):
            return (me ^ k) * zs + z + offset_of(s)

        def key_copies(s):
            for k in range(spans):
                at = pl.multiple_of(block(s, k) * tile, tile)
                to = keys_out.at[0, :, :, pl.ds(at, tile)]
                yield pltpu.make_async_copy(key_s.at[s, k], to, sems.at[s, k, 0])

        def value_copies(s):
            for k in range(spans):
                at = pl.multiple_of(block(s, k) * tile * heads, tile * heads)
                to = values_out.at[pl.ds(at, tile * heads)]
                yield pltpu.make_async_copy(value_s.at[s, k], to, sems.at[s, k, 1])

        def work(s, base):
            k = 0
            for j, chunk in enumerate(slots[s][1]):
                own, other = ins[base + 2 * j], ins[base + 2 * j + 1]
                for b in range(chunk[0].shape[0]):
                    mine, theirs = own[b], other[b]
                    got = (jnp.where(first, mine, theirs), jnp.where(first, theirs, mine))
                    for c in range(CORES):
                        at = (k * CORES + c) * count
                        for i in range(pieces):
                            rows_s[at : at + count, i * LANES : (i + 1) * LANES] = got[c][
                                i * count : (i + 1) * count
                            ]
                        tail = got[c][pieces * count :].astype(jnp.float32)
                        for i in range(fold):
                            rot_s[at + i * cut : at + (i + 1) * cut] = tail[
                                :, i * rot : (i + 1) * rot
                            ].astype(jnp.bfloat16)
                    k += 1
            rows = rows_s[...]
            dims = (((1,), (1,)), ((), ()))
            wide_keys = lax.dot_general(keys_ref[...], rows, dims, preferred_element_type=jnp.float32)
            wide_keys = wide_keys.astype(jnp.bfloat16)
            eye = (
                lax.broadcasted_iota(jnp.int32, (rot, rot), 0)
                == lax.broadcasted_iota(jnp.int32, (rot, rot), 1)
            ).astype(jnp.float32).astype(jnp.bfloat16)
            shared = lax.dot_general(eye, rot_s[...], dims, preferred_element_type=jnp.float32)
            shared = shared.astype(jnp.bfloat16)
            for k in range(spans):
                lanes = slice(k * tile, (k + 1) * tile)
                for h in range(heads):
                    key_s[s, k, h, :key_part] = wide_keys[h * key_part : (h + 1) * key_part, lanes]
                    key_s[s, k, h, key_part:] = shared[:, lanes]
            for copy in key_copies(s):
                copy.start()
            wide_values = jnp.dot(rows, value_ref[...], preferred_element_type=jnp.float32)
            for h in range(heads):
                wide_s[pl.ds(h, every, stride=heads)] = wide_values[
                    :, h * value_size : (h + 1) * value_size
                ]
            for k in range(spans):
                value_s[s, k] = wide_s[k * tile * heads : (k + 1) * tile * heads].astype(jnp.bfloat16)
            for copy in value_copies(s):
                copy.start()

        base = 0
        for s, (_, chunks) in enumerate(slots):
            at = z + offset_of(s)
            there = (at >= 0) & (at < zs)
            pl.when(there)(lambda s=s, base=base: work(s, base))
            base += 2 * len(chunks)
        for s in range(len(slots)):
            at = z + offset_of(s)
            there = (at >= 0) & (at < zs)

            @pl.when(there)
            def _(s=s):
                for copy in (*key_copies(s), *value_copies(s)):
                    copy.wait()

    length = every * zs
    given = (*arrays, keys_t, values)
    if last:
        given = [pltpu.with_memory_space_constraint(a, pltpu.VMEM) for a in given]
    return pl.pallas_call(
        body,
        in_specs=[VMEM] * (len(arrays) + 2) + [HBM] * len(before),
        out_specs=[HBM, HBM],
        out_shape=[
            jax.ShapeDtypeStruct((1, heads, key_part + rot, length), jnp.bfloat16),
            jax.ShapeDtypeStruct((length * heads, value_size), jnp.bfloat16),
        ],
        scratch_shapes=[
            pltpu.VMEM((every, width), jnp.bfloat16),
            pltpu.VMEM((every, rot), jnp.bfloat16),
            pltpu.VMEM((every * heads, value_size), jnp.float32),
            pltpu.VMEM((len(slots), spans, heads, key_part + rot, tile), jnp.bfloat16),
            pltpu.VMEM((len(slots), spans, tile * heads, value_size), jnp.bfloat16),
            pltpu.SemaphoreType.DMA((len(slots), spans, 2)),
        ],
        input_output_aliases={len(arrays) + 2 + i: i for i in range(len(before))},
    )(*given, *before)


def expand_spans(order, chunks, keys_t, values, count, rot, width, spans):
    heads = values.shape[1]
    key_part = keys_t.shape[0] // heads
    value_size = values.shape[2]
    values = values.reshape(width, heads * value_size)
    zs, _, high, _ = chunks[0][0].shape
    cores = len(chunks[0])
    tile = zs * cores * count
    pieces, fold = width // LANES, LANES // rot
    cut = count // fold
    starts = [0]
    for chunk in chunks:
        starts.append(starts[-1] + chunk[0].shape[1])
    refs_of = len(chunks) * cores

    def body(order_ref, *refs):
        ins, (key_ref, value_ref, keys_out, values_out, rows_s, rot_s, wide_s) = (
            refs[:refs_of],
            refs[refs_of:],
        )
        step = pl.program_id(0)
        first = order_ref[spans] == 0

        for j in range(len(chunks)):

            @pl.when((step >= starts[j]) & (step < starts[j + 1]))
            def _(j=j):
                pair = ins[j * cores : (j + 1) * cores]
                for z in range(zs):
                    got = [ref[z, 0] for ref in pair]
                    if cores == 2:
                        got = [
                            jnp.where(first, got[0], got[1]),
                            jnp.where(first, got[1], got[0]),
                        ]
                    for c in range(cores):
                        at = (z * cores + c) * count
                        for i in range(pieces):
                            rows_s[at : at + count, i * LANES : (i + 1) * LANES] = got[c][
                                i * count : (i + 1) * count
                            ]
                        tail = got[c][pieces * count :].astype(jnp.float32)
                        for i in range(fold):
                            rot_s[at + i * cut : at + (i + 1) * cut] = tail[
                                :, i * rot : (i + 1) * rot
                            ].astype(jnp.bfloat16)

        rows = rows_s[...]
        dims = (((1,), (1,)), ((), ()))
        wide_keys = lax.dot_general(key_ref[...], rows, dims, preferred_element_type=jnp.float32)
        wide_keys = wide_keys.astype(jnp.bfloat16)
        eye = (
            lax.broadcasted_iota(jnp.int32, (rot, rot), 0)
            == lax.broadcasted_iota(jnp.int32, (rot, rot), 1)
        ).astype(jnp.float32).astype(jnp.bfloat16)
        shared = lax.dot_general(eye, rot_s[...], dims, preferred_element_type=jnp.float32)
        shared = shared.astype(jnp.bfloat16)
        for h in range(heads):
            keys_out[0, h, :key_part] = wide_keys[h * key_part : (h + 1) * key_part]
            keys_out[0, h, key_part:] = shared
        wide_values = jnp.dot(rows, value_ref[...], preferred_element_type=jnp.float32)
        if heads == 1:
            values_out[...] = wide_values.astype(jnp.bfloat16)
        else:
            for h in range(heads):
                wide_s[pl.ds(h, tile, stride=heads)] = wide_values[
                    :, h * value_size : (h + 1) * value_size
                ]
            values_out[...] = wide_s[...].astype(jnp.bfloat16)

    length = spans * tile
    specs = []
    for j, chunk in enumerate(chunks):
        most = chunk[0].shape[1] - 1
        for _ in chunk:
            specs.append(
                pl.BlockSpec(
                    (zs, 1, high, LANES),
                    lambda i, o, a=starts[j], m=most: (0, jnp.clip(i - a, 0, m), 0, 0),
                )
            )
    whole = lambda i, o: (0, 0)
    decode_keys, decode_values = pl.pallas_call(
        body,
        grid_spec=pltpu.PrefetchScalarGridSpec(
            num_scalar_prefetch=1,
            grid=(spans,),
            in_specs=specs
            + [pl.BlockSpec(keys_t.shape, whole), pl.BlockSpec(values.shape, whole)],
            out_specs=[
                pl.BlockSpec((1, heads, key_part + rot, tile), lambda i, o: (0, 0, 0, o[i])),
                pl.BlockSpec((tile * heads, value_size), lambda i, o: (o[i], 0)),
            ],
            scratch_shapes=[
                pltpu.VMEM((tile, width), jnp.bfloat16),
                pltpu.VMEM((tile, rot), jnp.bfloat16),
                pltpu.VMEM((tile * heads, value_size), jnp.float32),
            ],
        ),
        out_shape=[
            jax.ShapeDtypeStruct((1, heads, key_part + rot, length), jnp.bfloat16),
            jax.ShapeDtypeStruct((length * heads, value_size), jnp.bfloat16),
        ],
        name="expand_spans",
    )(order, *[a for chunk in chunks for a in chunk], keys_t, values)
    return decode_keys, decode_values.reshape(1, length, heads, value_size)


def decode(latents, rotary_rows, latent_gain, key_up, value_up):
    spans, models = lax.axis_size("span"), lax.axis_size("model")
    zs = models // CORES
    _, count, width = latents.shape
    rot = rotary_rows.shape[2]
    heads, key_part, value_size = key_up.shape[1], key_up.shape[2], value_up.shape[2]
    shape = (heads, key_part, value_size, count, rot, width, spans, zs)
    packed = pack_rows(latents, rotary_rows, latent_gain, spans)
    keys_t = key_up.transpose(1, 2, 0).reshape(-1, width)
    values = value_up.reshape(width, heads * value_size)
    swap = [(i, i ^ 1) for i in range(models)]

    parts = [packed[0]]
    for k in range(1, spans):
        parts.append(lax.ppermute(packed[k], "span", [(i, i ^ k) for i in range(spans)]))
    size = spans // CHUNKS
    keys_t, values, *parts[1:] = lax.optimization_barrier((keys_t, values, *parts[1:]))
    if (CORES * count) % LANES:
        me, place = lax.axis_index("span"), lax.axis_index("model")
        core = place % CORES
        order = jnp.concatenate(
            [me ^ jnp.arange(spans, dtype=jnp.int32), core.astype(jnp.int32)[None]]
        )
        along = [[z * CORES + c for z in range(zs)] for c in range(CORES)]
        mine = jnp.concatenate(parts, axis=0)
        own = lax.all_gather(mine, "model", axis_index_groups=along)
        chunks = [(own, lax.ppermute(own, "model", swap))]
        return expand_spans(order, chunks, keys_t, value_up, count, rot, width, spans)
    own = [jnp.concatenate(parts[j * size : (j + 1) * size], axis=0) for j in range(CHUNKS)]

    def steps(way, far):
        return [
            (z * CORES + c, (z + way) * CORES + c)
            for z in range(zs)
            if 0 <= z + way < zs and 0 <= z - way * far < zs
            for c in range(CORES)
        ]

    def paired(x):
        return (x, lax.ppermute(x, "model", swap))

    z = lax.axis_index("model") // CORES
    up = down = merged = own[0]
    slots = [[(0, [paired(own[0])])]]
    for d in range(1, zs):
        if merged is not up:
            merged = lax.ppermute(merged, "model", steps(1, d - 1) + steps(-1, d - 1))
        else:
            up = lax.ppermute(up, "model", steps(1, d - 1))
            down = lax.ppermute(down, "model", steps(-1, d - 1))
            merged = jnp.where(z >= d, up, down) if 2 * d >= zs else up
        if 2 * d >= zs:
            slots.append([((-d, d), [paired(merged)])])
        else:
            slots.append([(-d, [paired(up)]), (d, [paired(down)])])
    groups = [sum(slots[:-1], []), slots[-1]]
    outs = ()
    for n, group in enumerate(groups):
        outs = expand(group, outs, keys_t, values, shape, n == 1)
    decode_keys, decode_values = outs
    return decode_keys, decode_values.reshape(1, -1, heads, value_size)


def solution(mesh):
    placed = (
        P(None, ("span", "model"), None),
        P(None, ("span", "model"), None),
        P(),
        P(None, "model", None),
        P(None, "model", None),
    )
    return jax.shard_map(
        decode,
        mesh=mesh,
        in_specs=placed,
        out_specs=(P("span", "model", None, None), P("span", None, "model", None)),
        check_vma=False,
    )
```
